256 devices in a mesh: tm: 128 (over y, x, z), head: 2 (over core).
Axes of the slice: x: 4, y: 4, z: 8, core: 2. Of those that a mesh axis runs over, the one named last changes fastest.
Arguments:
- queries: bfloat16 [16384, 4096], P('tm', 'head'), may hold values from -6 to 6
- keys: bfloat16 [16384, 4096], P('tm', 'head'), may hold values from -6 to 6
- values: bfloat16 [16384, 4096], P('tm', 'head'), may hold values from -6 to 6
- segment: int32 [16384], P('tm'), may hold values from 0 to 1, never falling along the last dimension, each value on 1 to 14336 neighbouring positions
- level_weight: float32 [15, 32, 16384], P(None, 'head', 'tm'), may hold values from 0.16 to 6
- gain: float32 [4096], P('head'), may hold values from 0.1 to 1.9
- grad_out: bfloat16 [16384, 4096], P('tm', 'head'), may hold values from -6 to 6
Outputs:
- normed: bfloat16 [16384, 4096], P('tm', 'head')
- grad_queries: bfloat16 [16384, 4096], P('tm', 'head')
- grad_keys: bfloat16 [16384, 4096], P('tm', 'head')
- grad_values: bfloat16 [16384, 4096], P('tm', 'head')
- grad_level: float32 [15, 32, 16384], P(None, 'head', 'tm')
The draws below stay inside these ranges and needn't reach their ends.
Inputs may be any that keep to these rules, and one draw needn't show every extreme that they name: segment numbers never fall along the sequence; each of the two segments holds 2048 to 14336 neighbouring positions.
All inputs are finite; a program needn't handle non-finite values.
Results may differ from the reference program's by a relative error of at most 0.0055.
Values sent between devices are 32-bit elements; how exact they have to be, the bound alone decides.
A program may use at most 128 MiB of HBM per device.

```python
import math
import jax
import jax.numpy as jnp
import numpy as np
from jax import lax

HEADS = 32
HEAD_DIM = 128
TOK_DEV = 128
TOKENS = 16384
FEAT = 4096
LEVELS = 15
N_TM = 128


def draw_level_weight(key, part):
    ramp = jnp.arange(HEADS, dtype=jnp.float32) / (HEADS - 1) - 0.5
    head_scale = jnp.exp(jnp.log(3.0) * ramp)
    spread = jnp.exp(jax.random.uniform(key, (LEVELS, HEADS, TOKENS), jnp.float32, jnp.log(0.5), jnp.log(2.0)))
    return spread * head_scale[None, :, None]


def steps_of(stream_key, dims, cuts, least, largest):
    def one(axis_at, parts):
        steps = jax.random.uniform(jax.random.fold_in(jax.random.fold_in(stream_key, 6), axis_at), (parts,), jnp.float32, least / len(cuts), largest / len(cuts))
        return jnp.repeat(jnp.exp(steps), dims[axis_at] // parts).reshape((-1,) + (1,) * (len(dims) - axis_at - 1))

    level = one(*cuts[0])
    for cut in cuts[1:]:
        level = level * one(*cut)
    return level


def profile(number_of, total, limit, lean):
    portions = [(1 << 20) // math.isqrt(rank ** lean) + 1 for rank in range(2, number_of + 1)]
    spare, holding = total - limit - (number_of - 1), [1] * (number_of - 1)
    while spare > 0:
        free = [i for i in range(number_of - 1) if holding[i] < limit]
        mass, left = sum([portions[i] for i in free]), spare
        for i in free:
            addition = min(limit - holding[i], max(1, left * portions[i] // mass), spare)
            holding[i] = holding[i] + addition
            spare = spare - addition
    return np.array([limit] + holding)


def uneven(stream_key, number_of, total, reach, skew):
    if number_of == 2:
        one = jax.random.randint(stream_key, (), max(1, total - reach), min(reach, total - 1) + 1)
        return jnp.stack([one, total - one])
    lengths = jnp.asarray(profile(number_of, total, reach, skew), jnp.int32)
    pairs = (number_of - 1) // 2
    giver, taker = lengths[1:1 + 2 * pairs:2], lengths[2:2 + 2 * pairs:2]
    room = jnp.minimum(giver - 1, reach - taker)
    passed = jax.random.randint(jax.random.fold_in(stream_key, 1), (pairs,), 0, 1 << 20) % (room + 1)
    lengths = lengths.at[1:1 + 2 * pairs:2].set(giver - passed).at[2:2 + 2 * pairs:2].set(taker + passed)
    return lengths[jax.random.permutation(jax.random.fold_in(stream_key, 2), number_of)]


def scatter_about(own_key, extent, scale, bound, shards=(), kind=jnp.bfloat16):
    drawn = scale * jax.random.normal(own_key, extent, jnp.float32)
    if shards:
        drawn = drawn * steps_of(own_key, extent, shards, -0.22, 0.18)
    return jnp.clip(drawn, -bound, bound).astype(kind)


def setup_inputs(seed: int = 0) -> dict:
    key_list = jax.random.split(jax.random.key(seed), 8)
    queries = scatter_about(key_list[0], (TOKENS, FEAT), 1.0, 6.0, ((0, 128), (1, 2)))
    keys = scatter_about(key_list[1], (TOKENS, FEAT), 1.0, 6.0, ((0, 128), (1, 2)))
    values = scatter_about(key_list[2], (TOKENS, FEAT), 1.0, 6.0, ((0, 128), (1, 2)))
    segment = jnp.searchsorted(jnp.cumsum(uneven(key_list[3], 2, TOKENS, TOKENS - TOKENS // 8, 2)), jnp.arange(TOKENS), side="right").astype(jnp.int32)
    level_weight = draw_level_weight(jax.random.fold_in(key_list[7], 71), 0)
    gain = jnp.clip(1.0 + 0.18 * jax.random.normal(key_list[5], (FEAT,), jnp.float32), 0.1, 1.9)
    grad_out = scatter_about(key_list[6], (TOKENS, FEAT), 1.0, 6.0, ((0, 128), (1, 2)))
    return {"queries": queries, "keys": keys, "values": values, "segment": segment, "level_weight": level_weight, "gain": gain, "grad_out": grad_out}


EPSILON = 1e-05
PRECISE = lax.Precision.HIGHEST

def level_table(tokens):
    places = jnp.arange(tokens, dtype=jnp.int32)
    crossed = jnp.bitwise_xor(places[:, None], places[None, :])
    levels = jnp.zeros((tokens, tokens), jnp.int32)
    for offset in range(tokens.bit_length() - 1):
        levels = levels + (jnp.right_shift(crossed, offset) > 0).astype(jnp.int32)
    return (levels, places[:, None] >= places[None, :])

def near_weight(block_scaled, block_segment, levels, causal, local_levels):
    same_segment = (block_segment[:, None] == block_segment[None, :]) & causal
    weight = jnp.zeros((block_scaled.shape[1],) + levels.shape, jnp.float32)
    for tier_level in range(local_levels):
        weight = weight + jnp.where(levels == tier_level, block_scaled[tier_level][:, :, None], jnp.float32(0.0))
    return (jnp.where(same_segment[None], weight, jnp.float32(0.0)), same_segment)

def reference(queries, keys, values, segment, level_weight, gain, grad_out):
    tokens = TOK_DEV
    blocks = N_TM
    head_count = HEADS
    head_width = HEAD_DIM
    log_tm = blocks.bit_length() - 1
    local_levels = tokens.bit_length()
    features = head_count * head_width
    levels, causal = level_table(tokens)
    level_scale = jnp.exp2(-jnp.maximum(jnp.arange(LEVELS) - 1, 0).astype(jnp.float32) / 2.0)
    scaled = level_weight * level_scale[:, None, None]
    shape4 = (blocks, tokens, head_count, head_width)
    query_blocks = queries.reshape(shape4)
    key_blocks = keys.reshape(shape4)
    value_blocks = values.reshape(shape4)
    grad_blocks = grad_out.reshape(blocks, tokens, features)
    segment_blocks = segment.reshape(blocks, tokens)
    scaled_blocks = scaled.reshape(LEVELS, head_count, blocks, tokens).transpose(2, 0, 1, 3)
    block_lasts = segment_blocks[:, -1]
    block_numbers = jnp.arange(blocks, dtype=jnp.int32)

    def tail_of(pieces):
        key_block, value_block, block_segment = pieces
        keep_rows = (block_segment == block_segment[-1]).astype(jnp.float32)
        return jnp.einsum('shd,she->hde', key_block.astype(jnp.float32) * keep_rows[:, None, None], value_block.astype(jnp.float32), precision=PRECISE)
    tails = lax.map(tail_of, (key_blocks, value_blocks, segment_blocks))
    group_totals = []
    group_ends = []
    for level_bit in range(log_tm):
        group_size = 2 ** level_bit
        lasts_grouped = block_lasts.reshape(blocks // group_size, group_size)
        end_gates = lasts_grouped[:, -1]
        chosen = (lasts_grouped == end_gates[:, None]).astype(jnp.float32)
        grouped = tails.reshape(blocks // group_size, group_size, head_count, head_width, head_width)
        group_totals.append(jnp.einsum('gm,gmhde->ghde', chosen, grouped, precision=PRECISE))
        group_ends.append(end_gates)

    def block_step(accumulated, pieces):
        query_block, key_block, value_block, grad_block, block_segment, block_scaled, block_index = pieces
        query_float = query_block.astype(jnp.float32)
        key_float = key_block.astype(jnp.float32)
        value_float = value_block.astype(jnp.float32)
        weight, same_segment = near_weight(block_scaled, block_segment, levels, causal, local_levels)
        scores = jnp.einsum('thd,shd->hts', query_float, key_float, precision=PRECISE)
        near_terms = (scores * weight).astype(jnp.bfloat16).astype(jnp.float32)
        mixed_out = jnp.einsum('hts,shd->thd', near_terms, value_float, precision=PRECISE)
        reaches = []
        weighted_all = []
        reads = []
        bucket_all = []
        for level_bit in range(log_tm):
            group_index = jnp.right_shift(block_index, level_bit)
            is_upper = group_index % 2 == 1
            partner = jnp.bitwise_xor(group_index, 1)
            bucket = group_totals[level_bit][partner]
            gate_value = group_ends[level_bit][partner]
            reach_mask = jnp.where(is_upper & (block_segment == gate_value), jnp.float32(1.0), jnp.float32(0.0))
            weighted = reach_mask[:, None] * block_scaled[local_levels + level_bit].T
            remote_read = jnp.einsum('thd,hde->the', query_float, bucket, precision=PRECISE)
            mixed_out = mixed_out + remote_read * weighted[:, :, None]
            reaches.append(reach_mask)
            weighted_all.append(weighted)
            reads.append(remote_read)
            bucket_all.append(bucket)
        flat_out = mixed_out.reshape(tokens, features)
        radius = jnp.sqrt(lax.optimization_barrier(jnp.mean(flat_out * flat_out, axis=1)) + EPSILON)
        normed = (flat_out / radius[:, None] * gain).astype(jnp.bfloat16)
        grad_float = grad_block.astype(jnp.float32)
        project = lax.optimization_barrier(jnp.sum(gain * grad_float * flat_out, axis=1))
        grad_mixed = (gain * grad_float / radius[:, None] - flat_out * (project / (features * radius ** 3))[:, None]).astype(jnp.bfloat16)
        grad_heads = grad_mixed.astype(jnp.float32).reshape(tokens, head_count, head_width)
        grad_near = jnp.einsum('thd,shd->hts', grad_heads, value_float, precision=PRECISE)
        grad_score = (grad_near * weight).astype(jnp.bfloat16).astype(jnp.float32)
        grad_query = jnp.einsum('hts,shd->thd', grad_score, key_float, precision=PRECISE)
        grad_key = jnp.einsum('hts,thd->shd', grad_score, query_float, precision=PRECISE)
        grad_value = jnp.einsum('hts,thd->shd', near_terms, grad_heads, precision=PRECISE)
        masked = jnp.where(same_segment[None], grad_near * scores, jnp.float32(0.0))
        level_rows = [lax.optimization_barrier(jnp.sum(jnp.where(levels == tier_level, masked, jnp.float32(0.0)), axis=2)) for tier_level in range(local_levels)]
        updated = []
        for level_bit in range(log_tm):
            grad_query = grad_query + jnp.einsum('hde,the->thd', bucket_all[level_bit], grad_heads, precision=PRECISE) * weighted_all[level_bit][:, :, None]
            level_rows.append(reaches[level_bit][None, :] * lax.optimization_barrier(jnp.sum(reads[level_bit] * grad_heads, axis=2)).T)
            grad_bucket = jnp.einsum('thd,the->hde', query_float * weighted_all[level_bit][:, :, None], grad_heads, precision=PRECISE)
            updated.append(accumulated[level_bit].at[jnp.right_shift(block_index, level_bit)].add(grad_bucket))
        grad_level = jnp.stack(level_rows) * level_scale[:, None, None]
        return (updated, (normed, grad_query.astype(jnp.bfloat16), grad_key, grad_value, grad_level))
    initial = [jnp.zeros((blocks >> level_bit, head_count, head_width, head_width), jnp.float32) for level_bit in range(log_tm)]
    accumulated, outputs = lax.scan(block_step, initial, (query_blocks, key_blocks, value_blocks, grad_blocks, segment_blocks, scaled_blocks, block_numbers))
    normed, grad_query, partial_key, partial_value, grad_level = outputs

    def finish(pieces):
        key_block, value_block, block_segment, block_index, key_part, value_part = pieces
        grad_tail = jnp.zeros((head_count, head_width, head_width), jnp.float32)
        for level_bit in range(log_tm):
            group_index = jnp.right_shift(block_index, level_bit)
            is_lower = group_index % 2 == 0
            joined = is_lower & (block_segment[-1] == group_ends[level_bit][group_index])
            grad_tail = grad_tail + jnp.where(joined, accumulated[level_bit][jnp.bitwise_xor(group_index, 1)], jnp.float32(0.0))
        keep_rows = (block_segment == block_segment[-1]).astype(jnp.float32)[:, None, None]
        key_grad = key_part + keep_rows * jnp.einsum('hde,she->shd', grad_tail, value_block.astype(jnp.float32), precision=PRECISE)
        value_grad = value_part + keep_rows * jnp.einsum('hde,shd->she', grad_tail, key_block.astype(jnp.float32), precision=PRECISE)
        return (key_grad.astype(jnp.bfloat16), value_grad.astype(jnp.bfloat16))
    grad_keys, grad_values = lax.map(finish, (key_blocks, value_blocks, segment_blocks, block_numbers, partial_key, partial_value))
    total = blocks * tokens
    return (normed.reshape(total, features), grad_query.reshape(total, features), grad_keys.reshape(total, features), grad_values.reshape(total, features), grad_level.transpose(1, 2, 0, 3).reshape(LEVELS, head_count, total))
```

```python
import functools
import jax
import jax.numpy as jnp
from jax import lax
from jax.experimental import pallas as pl
from jax.experimental.pallas import tpu as pltpu
from jax.sharding import PartitionSpec as P

MESH = pl.DeviceIdType.MESH
F32 = jnp.float32
BF16 = jnp.bfloat16
EPSILON = 1e-05
TOK = 128
WIDTH = 128
NH = 16
BITS = 7
NEAR_LEVELS = 8
LEVELS = NEAR_LEVELS + BITS
FEATURES = 4096
UP_LAG = (0, 3, 7, 10, 12, 14, 16)
DOWN_LAG = (0, 1, 3, 5, 7, 9, 11, 13, 15, 17)


def dot(a, b, left, right):
    return lax.dot_general(a, b, (((left,), (right,)), ((), ())), preferred_element_type=F32)


def place():
    tm = lax.axis_index("tm")
    z = lax.rem(tm, 8)
    x = lax.rem(lax.div(tm, 8), 4)
    y = lax.div(tm, 32)
    inner = lax.rem(lax.div(z + 1, 2), 2)
    near = tm + 1 - 2 * lax.rem(z, 2)
    across = tm - z + inner * (8 * lax.div(z, 4) + 3 - z) + (1 - inner) * (7 - z)
    x_one = tm + 8 * (1 - 2 * lax.rem(x, 2))
    x_three = tm + 8 * (3 - 2 * x)
    y_one = tm + 32 * (1 - 2 * lax.rem(y, 2))
    y_three = tm + 32 * (3 - 2 * y)
    bits = (
        lax.rem(z, 2), lax.rem(lax.div(z, 2), 2), lax.div(z, 4),
        lax.rem(x, 2), lax.div(x, 2), lax.rem(y, 2), lax.div(y, 2),
    )
    return inner, (near, across, x_one, x_three, y_one, y_three), bits


def remote(src, dst, send, recv, other):
    return pltpu.make_async_remote_copy(
        src_ref=src, dst_ref=dst, send_sem=send, recv_sem=recv,
        device_id=other, device_id_type=MESH,
    )


def body(
    q, k, v, g, lw, rows, table, keep, gain,
    normed, gq, gk, gv, gl,
    tails, recv, agg, grecv, gagg, reach, q_t, near, score, weight, mixed, sums, sums_got,
    gm, o, got, got_join, cur, gkp, gvp,
    ssem, rsem, lsem, gss, grs, gls, dssem, drsem, jss, jrs, xss, xrs,
):
    inner, partners, bits = place()
    near_by, across, x_one, x_three, y_one, y_three = partners
    other_core = {"head": 1 - lax.axis_index("head")}
    target = tuple(
        {"tm": p} for p in (near_by, across, across, x_one, x_three, y_one, y_three)
    )
    is_inner = inner == 1
    is_outer = inner == 0
    upper = tuple(bit == 1 for bit in bits)
    lower = tuple(bit == 0 for bit in bits)
    upper_f = tuple(bit.astype(F32) for bit in bits)

    barrier = pltpu.get_barrier_semaphore()
    for p in partners:
        pl.semaphore_signal(barrier, inc=1, device_id={"tm": p}, device_id_type=MESH)
    pl.semaphore_signal(barrier, inc=1, device_id=other_core, device_id_type=MESH)
    pl.semaphore_wait(barrier, 7)

    def cols(h):
        return pl.ds(pl.multiple_of(h * WIDTH, WIDTH), WIDTH)

    def only(b, fn):
        if b == 1:
            pl.when(is_inner)(fn)
        elif b == 2:
            pl.when(is_outer)(fn)
        else:
            fn()

    def up_copy(b, h):
        src = tails.at[h] if b == 0 else agg.at[b - 1, h]
        return remote(src, recv.at[b, h], ssem.at[b, h], rsem.at[b, h], target[b])

    def up_relay(b, h):
        return remote(recv.at[b, h], recv.at[b, h], lsem.at[h], rsem.at[b, h], target[0])

    def gate_copy(b):
        return remote(gagg.at[b], grecv.at[b], gss.at[b], grs.at[b], target[b])

    def gate_relay(b):
        return remote(grecv.at[b], grecv.at[b], gls, grs.at[b], target[0])

    gagg[0] = rows[0]
    gate_copy(0).start()

    @pl.loop(0, NH)
    def _(h):
        kept = k[:, cols(h)].astype(F32) * keep[...]
        tails[h] = dot(kept.astype(BF16), v[:, cols(h)], 0, 0)
        up_copy(0, h).start()

    def near_forward(h):
        query = q[:, cols(h)]
        s = dot(k[:, cols(h)], query, 1, 1)
        level = table[...]
        w = jnp.zeros((TOK, TOK), F32)
        for l in range(NEAR_LEVELS):
            w = jnp.where(level == float(l), lw[h, l:l + 1, :], w)
        terms = (s * w).astype(BF16)
        score[h] = s
        weight[h] = w
        near[h] = terms
        q_t[h] = query.T
        mixed[h] = dot(terms, v[:, cols(h)], 0, 0)

    def up_event(b, h):
        @pl.when(h == 0)
        def _():
            gate_copy(b).wait_recv()
            if b in (1, 2):
                only(b, lambda: gate_relay(b).start())
            if b < BITS - 1:
                gagg[b + 1] = gagg[b] * upper_f[b] + grecv[b] * (1.0 - upper_f[b])
                only(b + 1, lambda: gate_copy(b + 1).start())
            hit = jnp.where(rows[1, 0:1, :] == grecv[b, 0:1, :], 1.0, 0.0)
            reach[b:b + 1, :] = hit * upper_f[b]

        up_copy(b, h).wait_recv()
        if b in (1, 2):
            only(b, lambda: up_relay(b, h).start())
        if b < BITS - 1:
            same = jnp.where(grecv[b, 0:1, :] == gagg[b, 0:1, :], 1.0, 0.0)
            mine_by = upper_f[b] + (1.0 - upper_f[b]) * same
            got_by = (1.0 - upper_f[b]) + upper_f[b] * same
            mine = tails[h] if b == 0 else agg[b - 1, h]
            agg[b, h] = mine * mine_by + recv[b, h] * got_by
            only(b + 1, lambda: up_copy(b + 1, h).start())

    def far_read(h):
        by = lw[h, 8:16, :] * reach[...]
        by_t = by.T
        query = q[:, cols(h)].astype(F32)
        for b in range(BITS):
            @pl.when(upper[b])
            def _(b=b):
                scaled_q = (query * by_t[:, b:b + 1]).astype(BF16)
                mixed[h] = mixed[h] + dot(scaled_q, recv[b, h].astype(BF16), 1, 0)
        m = mixed[h]
        sums[0] = sums[0] + m * m
        sums[1] = sums[1] + m * g[:, cols(h)].astype(F32) * gain[:, cols(h)]

    sums[...] = jnp.zeros_like(sums)
    reach[...] = jnp.zeros_like(reach)

    @pl.loop(0, NH + UP_LAG[-1])
    def _(step):
        for b in range(BITS):
            h = step - UP_LAG[b]

            @pl.when((h >= 0) & (h < NH))
            def _(b=b, h=h):
                up_event(b, h)

        @pl.when(step < NH)
        def _():
            near_forward(step)

        h = step - UP_LAG[-1]

        @pl.when(h >= 0)
        def _():
            far_read(h)

    swap = remote(sums, sums_got, xss, xrs, other_core)
    swap.start()
    swap.wait_recv()
    squares = jnp.sum(sums[0] + sums_got[0], axis=1, keepdims=True)
    project = jnp.sum(sums[1] + sums_got[1], axis=1, keepdims=True)
    radius = jnp.sqrt(squares / FEATURES + EPSILON)
    inverse = 1.0 / radius
    pull = project * inverse * inverse * inverse / FEATURES

    def down_copy(b, h):
        return remote(o.at[b, h], got.at[b, h], dssem.at[b, h], drsem.at[b, h], target[b])

    def join(b, h):
        return remote(o.at[b, h], got_join.at[h], jss.at[h], jrs.at[h], target[0])

    def far_row(b, h):
        return lw[h, 8 + b:9 + b, :] * reach[b:b + 1, :]

    def far_grad(b, h):
        scaled_q = (q_t[h].astype(F32) * far_row(b, h)).astype(BF16)
        return dot(scaled_q, gm[h], 1, 0)

    def split(b, h):
        same = jnp.where(grecv[b, 0:1, :] == gagg[b, 0:1, :], 1.0, 0.0)

        @pl.when(upper[b])
        def _():
            o[b, h] = cur[h] * same + far_grad(b, h)

        @pl.when(lower[b])
        def _():
            o[b, h] = cur[h]
            cur[h] = cur[h] * same

    def emit(h):
        m = mixed[h]
        scale = gain[:, cols(h)]
        normed[:, cols(h)] = (m * inverse * scale).astype(BF16)
        gm[h] = (scale * g[:, cols(h)].astype(F32) * inverse - m * pull).astype(BF16)

        @pl.when(upper[6])
        def _():
            o[6, h] = far_grad(6, h)
            down_copy(6, h).start()

    def top(h):
        @pl.when(lower[6])
        def _():
            down_copy(6, h).wait_recv()
            cur[h] = got[6, h]

        @pl.when(upper[6])
        def _():
            cur[h] = jnp.zeros((WIDTH, WIDTH), F32)

        split(5, h)
        down_copy(5, h).start()

    def middle(b, h):
        down_copy(b, h).wait_recv()
        cur[h] = cur[h] + got[b, h]
        split(b - 1, h)
        down_copy(b - 1, h).start()

    def three(h):
        down_copy(3, h).wait_recv()
        cur[h] = cur[h] + got[3, h]
        split(2, h)

        @pl.when(is_inner)
        def _():
            join(2, h).start()
            split(1, h)

    def two_join(h):
        @pl.when(is_outer)
        def _():
            join(2, h).wait_recv()
            o[2, h] = o[2, h] + got_join[h]
            down_copy(2, h).start()

    def two(h):
        @pl.when(is_outer)
        def _():
            down_copy(2, h).wait_recv()
            cur[h] = cur[h] + got[2, h]
            split(1, h)
            join(1, h).start()
            split(0, h)
            down_copy(0, h).start()

    def one_join(h):
        @pl.when(is_inner)
        def _():
            join(1, h).wait_recv()
            o[1, h] = o[1, h] + got_join[h]
            down_copy(1, h).start()

    def one(h):
        @pl.when(is_inner)
        def _():
            down_copy(1, h).wait_recv()
            cur[h] = cur[h] + got[1, h]
            split(0, h)
            down_copy(0, h).start()

    def near_backward(h):
        grad = gm[h]
        query = q[:, cols(h)]
        gn = dot(v[:, cols(h)], grad, 1, 1)
        gs = (gn * weight[h]).astype(BF16)
        gkp[h] = dot(gs, query, 1, 0)
        gvp[h] = dot(near[h], grad, 1, 0)
        both = gn * score[h]
        level = table[...]
        for l in range(NEAR_LEVELS):
            part = jnp.sum(jnp.where(level == float(l), both, 0.0), axis=0, keepdims=True)
            gl[l, pl.ds(h, 1), :] = part * (2.0 ** (-max(l - 1, 0) / 2))
        mixed[h] = jnp.zeros((WIDTH, TOK), F32)
        query_t = q_t[h].astype(F32)
        for b in range(BITS):
            gl[NEAR_LEVELS + b, pl.ds(h, 1), :] = jnp.zeros((1, TOK), F32)

            @pl.when(upper[b])
            def _(b=b):
                read = dot(recv[b, h].astype(BF16), grad, 1, 1)
                mixed[h] = mixed[h] + read * far_row(b, h)
                part = jnp.sum(query_t * read, axis=0, keepdims=True) * reach[b:b + 1, :]
                gl[NEAR_LEVELS + b, pl.ds(h, 1), :] = part * (2.0 ** (-(7 + b) / 2))
        gq[:, cols(h)] = (dot(gs, k[:, cols(h)], 0, 0) + mixed[h].T).astype(BF16)

    def zero(h):
        down_copy(0, h).wait_recv()
        carried = (cur[h] + got[0, h]).astype(BF16)
        held = keep[...]
        kept_v = (v[:, cols(h)].astype(F32) * held).astype(BF16)
        kept_k = (k[:, cols(h)].astype(F32) * held).astype(BF16)
        gk[:, cols(h)] = (gkp[h] + dot(kept_v, carried, 1, 1)).astype(BF16)
        gv[:, cols(h)] = (gvp[h] + dot(kept_k, carried, 1, 0)).astype(BF16)

    events = (
        emit, top, functools.partial(middle, 5), functools.partial(middle, 4), three,
        two_join, two, one_join, one, zero,
    )

    @pl.loop(0, NH + DOWN_LAG[-1])
    def _(step):
        for lag, event in zip(DOWN_LAG, events):
            h = step - lag

            @pl.when((h >= 0) & (h < NH))
            def _(h=h, event=event):
                event(h)

        h = step - 1

        @pl.when((h >= 0) & (h < NH))
        def _():
            near_backward(h)

    swap.wait_send()
    for b in range(BITS):
        only(b, lambda b=b: gate_copy(b).wait_send())
    gate_relay(1).wait_send()

    @pl.loop(0, NH)
    def _(h):
        for b in range(BITS):
            only(b, lambda b=b: up_copy(b, h).wait_send())
        up_relay(1, h).wait_send()
        for b in (0, 3, 4, 5):
            down_copy(b, h).wait_send()
        pl.when(upper[6])(lambda: down_copy(6, h).wait_send())
        pl.when(is_outer)(lambda: down_copy(2, h).wait_send())
        pl.when(is_inner)(lambda: down_copy(1, h).wait_send())
        join(1, h).wait_send()


def per_device(queries, keys, values, segment, level_weight, gain, grad_out):
    segment = segment.astype(F32)
    places = jnp.arange(TOK, dtype=jnp.int32)
    crossed = jnp.bitwise_xor(places[:, None], places[None, :])
    levels = jnp.zeros((TOK, TOK), F32)
    for offset in range(NEAR_LEVELS - 1):
        levels = levels + (jnp.right_shift(crossed, offset) > 0).astype(F32)
    seen = (segment[:, None] == segment[None, :]) & (places[:, None] <= places[None, :])
    table = jnp.where(seen, levels, -1.0)
    keep = jnp.broadcast_to(jnp.where(segment == segment[-1], 1.0, 0.0)[:, None], (TOK, WIDTH))
    rows = jnp.stack([
        jnp.broadcast_to(segment[-1:], (8, TOK)), jnp.broadcast_to(segment[None, :], (8, TOK)),
    ])
    level_scale = jnp.exp2(-jnp.maximum(jnp.arange(LEVELS) - 1, 0).astype(F32) / 2.0)
    scaled = level_weight * level_scale[:, None, None]
    by_head = jnp.pad(scaled, ((0, 1), (0, 0), (0, 0))).transpose(1, 0, 2)

    vmem = pl.BlockSpec(memory_space=pltpu.VMEM)
    dma = pltpu.SemaphoreType.DMA
    square = (WIDTH, WIDTH)
    wide = jax.ShapeDtypeStruct((TOK, NH * WIDTH), BF16)
    return pl.pallas_call(
        body,
        name="levels",
        out_shape=(wide, wide, wide, wide, jax.ShapeDtypeStruct((LEVELS, NH, TOK), F32)),
        in_specs=[vmem] * 9,
        out_specs=(vmem,) * 5,
        scratch_shapes=[
            pltpu.VMEM((NH,) + square, F32),
            pltpu.VMEM((BITS, NH) + square, F32),
            pltpu.VMEM((BITS - 1, NH) + square, F32),
            pltpu.VMEM((BITS, 8, 128), F32),
            pltpu.VMEM((BITS, 8, 128), F32),
            pltpu.VMEM((8, 128), F32),
            pltpu.VMEM((NH,) + square, BF16),
            pltpu.VMEM((NH,) + square, BF16),
            pltpu.VMEM((NH,) + square, F32),
            pltpu.VMEM((NH,) + square, F32),
            pltpu.VMEM((NH,) + square, F32),
            pltpu.VMEM((2,) + square, F32),
            pltpu.VMEM((2,) + square, F32),
            pltpu.VMEM((NH,) + square, BF16),
            pltpu.VMEM((BITS, NH) + square, F32),
            pltpu.VMEM((BITS, NH) + square, F32),
            pltpu.VMEM((NH,) + square, F32),
            pltpu.VMEM((NH,) + square, F32),
            pltpu.VMEM((NH,) + square, F32),
            pltpu.VMEM((NH,) + square, F32),
            dma((BITS, NH)), dma((BITS, NH)), dma((NH,)), dma((BITS,)), dma((BITS,)), dma,
            dma((BITS, NH)), dma((BITS, NH)), dma((NH,)), dma((NH,)), dma, dma,
        ],
        compiler_params=pltpu.CompilerParams(
            collective_id=1, has_side_effects=True, vmem_limit_bytes=56 << 20),
    )(queries, keys, values, grad_out, by_head, rows, table, keep, gain[None, :])


def solution(mesh):
    placed = (
        P("tm", "head"), P("tm", "head"), P("tm", "head"), P("tm"),
        P(None, "head", "tm"), P("head"), P("tm", "head"),
    )
    return jax.shard_map(
        per_device,
        mesh=mesh,
        in_specs=placed,
        out_specs=(P("tm", "head"),) * 4 + (P(None, "head", "tm"),),
        check_vma=False,
    )
```

```python
import functools
import jax
import jax.numpy as jnp
from jax import lax
from jax.experimental import pallas as pl
from jax.experimental.pallas import tpu as pltpu
from jax.sharding import PartitionSpec as P

MESH = pl.DeviceIdType.MESH
F32 = jnp.float32
BF16 = jnp.bfloat16
EPSILON = 1e-05
TOK = 128
WIDTH = 128
NH = 16
BITS = 7
NEAR_LEVELS = 8
LEVELS = NEAR_LEVELS + BITS
FEATURES = 4096
UP_LAG = (0, (2, 4), (8, 6), 10, 12, 14, 16)
AHEAD = 3
DOWN_LAG = (0, 2, 4, 6, 8, 10, 12, 14, 16, 18)


def level_scale(l):
    return 2.0 ** (-max(l - 1, 0) / 2)


def dot(a, b, left, right):
    return lax.dot_general(a, b, (((left,), (right,)), ((), ())), preferred_element_type=F32)


def place():
    tm = lax.axis_index("tm")
    z = lax.rem(tm, 8)
    x = lax.rem(lax.div(tm, 8), 4)
    y = lax.div(tm, 32)
    inner = lax.rem(lax.div(z + 1, 2), 2)
    near = tm + 1 - 2 * lax.rem(z, 2)
    across = tm - z + inner * (8 * lax.div(z, 4) + 3 - z) + (1 - inner) * (7 - z)
    x_one = tm + 8 * (1 - 2 * lax.rem(x, 2))
    x_three = tm + 8 * (3 - 2 * x)
    y_one = tm + 32 * (1 - 2 * lax.rem(y, 2))
    y_three = tm + 32 * (3 - 2 * y)
    bits = (
        lax.rem(z, 2), lax.rem(lax.div(z, 2), 2), lax.div(z, 4),
        lax.rem(x, 2), lax.div(x, 2), lax.rem(y, 2), lax.div(y, 2),
    )
    return inner, (near, across, x_one, x_three, y_one, y_three), bits


def remote(src, dst, send, recv, other):
    return pltpu.make_async_remote_copy(
        src_ref=src, dst_ref=dst, send_sem=send, recv_sem=recv,
        device_id=other, device_id_type=MESH,
    )


def body(
    q, k, v, g, lw, segment, gain,
    normed, gq, gk, gv, gl,
    table, keep, far, tails, recv, agg, grecv, gagg, reach, q_t, near, score, weight, mixed, sums, sums_got,
    gm, o, got, got_join, cur, gkp, gvp,
    ssem, rsem, lsem, gss, grs, gls, dssem, drsem, jss, jrs, xss, xrs,
):
    inner, partners, bits = place()
    near_by, across, x_one, x_three, y_one, y_three = partners
    other_core = {"head": 1 - lax.axis_index("head")}
    target = tuple(
        {"tm": p} for p in (near_by, across, across, x_one, x_three, y_one, y_three)
    )
    is_inner = inner == 1
    is_outer = inner == 0
    upper = tuple(bit == 1 for bit in bits)
    lower = tuple(bit == 0 for bit in bits)
    upper_f = tuple(bit.astype(F32) for bit in bits)

    barrier = pltpu.get_barrier_semaphore()
    for p in partners:
        pl.semaphore_signal(barrier, inc=1, device_id={"tm": p}, device_id_type=MESH)
    pl.semaphore_signal(barrier, inc=1, device_id=other_core, device_id_type=MESH)
    pl.semaphore_wait(barrier, 7)

    def cols(h):
        return pl.ds(pl.multiple_of(h * WIDTH, WIDTH), WIDTH)

    def only(b, fn):
        if b == 1:
            pl.when(is_inner)(fn)
        elif b == 2:
            pl.when(is_outer)(fn)
        else:
            fn()

    def up_copy(b, h):
        src = tails.at[h] if b == 0 else agg.at[b - 1, h]
        return remote(src, recv.at[b, h], ssem.at[b, h], rsem.at[b, h], target[b])

    def up_relay(b, h):
        return remote(recv.at[b, h], recv.at[b, h], lsem.at[h], rsem.at[b, h], target[0])

    def gate_copy(b):
        return remote(gagg.at[b], grecv.at[b], gss.at[b], grs.at[b], target[b])

    def gate_relay(b):
        return remote(grecv.at[b], grecv.at[b], gls, grs.at[b], target[0])

    def level_row(l, h):
        return lw[l, pl.ds(h, 1), :] * level_scale(l)

    def send_tail(h):
        kept = k[:, cols(h)].astype(F32) * keep[...]
        tails[h] = dot(kept.astype(BF16), v[:, cols(h)], 0, 0)
        up_copy(0, h).start()

    row = segment[...].astype(F32)
    last = row[:, TOK - 1:TOK]
    gagg[0] = jnp.broadcast_to(last, (8, TOK))
    gate_copy(0).start()
    across_t = jnp.broadcast_to(row, (TOK, TOK))
    down_s = across_t.T
    keep[...] = jnp.where(down_s == last, 1.0, 0.0)

    @pl.loop(0, AHEAD)
    def _(h):
        send_tail(h)

    at_s = lax.broadcasted_iota(jnp.int32, (TOK, TOK), 0)
    at_t = lax.broadcasted_iota(jnp.int32, (TOK, TOK), 1)
    crossed = jnp.bitwise_xor(at_s, at_t)
    levels = jnp.zeros((TOK, TOK), F32)
    for offset in range(NEAR_LEVELS - 1):
        levels = levels + jnp.where(crossed >= (1 << offset), 1.0, 0.0)
    table[...] = jnp.where((down_s == across_t) & (at_s <= at_t), levels, -1.0)

    def near_forward(h):
        query = q[:, cols(h)]
        s = dot(k[:, cols(h)], query, 1, 1)
        level = table[...]
        w = jnp.zeros((TOK, TOK), F32)
        for l in range(NEAR_LEVELS):
            w = jnp.where(level == float(l), level_row(l, h), w)
        terms = (s * w).astype(BF16)
        score[h] = s
        weight[h] = w
        near[h] = terms
        q_t[h] = query.T
        mixed[h] = dot(terms, v[:, cols(h)], 0, 0)

    def up_event(b, h):
        @pl.when(h == 0)
        def _():
            gate_copy(b).wait_recv()
            if b in (1, 2):
                only(b, lambda: gate_relay(b).start())
            if b < BITS - 1:
                gagg[b + 1] = gagg[b] * upper_f[b] + grecv[b] * (1.0 - upper_f[b])
                only(b + 1, lambda: gate_copy(b + 1).start())
            hit = jnp.where(segment[...].astype(F32) == grecv[b, 0:1, :], 1.0, 0.0)
            reach[b:b + 1, :] = hit * upper_f[b]

        up_copy(b, h).wait_recv()
        if b in (1, 2):
            only(b, lambda: up_relay(b, h).start())
        if b < BITS - 1:
            same = jnp.where(grecv[b, 0:1, :] == gagg[b, 0:1, :], 1.0, 0.0)
            mine_by = upper_f[b] + (1.0 - upper_f[b]) * same
            got_by = (1.0 - upper_f[b]) + upper_f[b] * same
            mine = tails[h] if b == 0 else agg[b - 1, h]
            agg[b, h] = mine * mine_by + recv[b, h] * got_by
            only(b + 1, lambda: up_copy(b + 1, h).start())

    def far_read(h):
        for b in range(BITS):
            far[b:b + 1, :] = level_row(NEAR_LEVELS + b, h)
        by_t = (far[...] * reach[...]).T
        query = q[:, cols(h)].astype(F32)
        for b in range(BITS):
            @pl.when(upper[b])
            def _(b=b):
                scaled_q = (query * by_t[:, b:b + 1]).astype(BF16)
                mixed[h] = mixed[h] + dot(scaled_q, recv[b, h].astype(BF16), 1, 0)
        m = mixed[h]
        sums[0] = sums[0] + m * m
        sums[1] = sums[1] + m * g[:, cols(h)].astype(F32) * gain[:, cols(h)]

    sums[...] = jnp.zeros_like(sums)
    reach[...] = jnp.zeros_like(reach)
    far[...] = jnp.zeros_like(far)

    @pl.loop(0, NH + UP_LAG[-1])
    def _(step):
        @pl.when(step + AHEAD < NH)
        def _():
            send_tail(step + AHEAD)

        for b in range(BITS):
            lag = UP_LAG[b]
            if isinstance(lag, tuple):
                lag = lag[0] * inner + lag[1] * (1 - inner)
            h = step - lag

            @pl.when((h >= 0) & (h < NH))
            def _(b=b, h=h):
                up_event(b, h)

        @pl.when(step < NH)
        def _():
            near_forward(step)

        h = step - UP_LAG[-1]

        @pl.when(h >= 0)
        def _():
            far_read(h)

    swap = remote(sums, sums_got, xss, xrs, other_core)
    swap.start()
    swap.wait_recv()
    squares = jnp.sum(sums[0] + sums_got[0], axis=1, keepdims=True)
    project = jnp.sum(sums[1] + sums_got[1], axis=1, keepdims=True)
    radius = jnp.sqrt(squares / FEATURES + EPSILON)
    inverse = 1.0 / radius
    pull = project * inverse * inverse * inverse / FEATURES

    def down_copy(b, h):
        return remote(o.at[b, h], got.at[b, h], dssem.at[b, h], drsem.at[b, h], target[b])

    def join(b, h):
        return remote(o.at[b, h], got_join.at[h], jss.at[h], jrs.at[h], target[0])

    def far_row(b, h):
        return level_row(NEAR_LEVELS + b, h) * reach[b:b + 1, :]

    def far_grad(b, h):
        scaled_q = (q_t[h].astype(F32) * far_row(b, h)).astype(BF16)
        return dot(scaled_q, gm[h], 1, 0)

    def split(b, h):
        same = jnp.where(grecv[b, 0:1, :] == gagg[b, 0:1, :], 1.0, 0.0)

        @pl.when(upper[b])
        def _():
            o[b, h] = cur[h] * same + far_grad(b, h)

        @pl.when(lower[b])
        def _():
            o[b, h] = cur[h]
            cur[h] = cur[h] * same

    def emit(h):
        m = mixed[h]
        scale = gain[:, cols(h)]
        normed[:, cols(h)] = (m * inverse * scale).astype(BF16)
        gm[h] = (scale * g[:, cols(h)].astype(F32) * inverse - m * pull).astype(BF16)

        @pl.when(upper[6])
        def _():
            o[6, h] = far_grad(6, h)
            down_copy(6, h).start()

    def top(h):
        @pl.when(lower[6])
        def _():
            down_copy(6, h).wait_recv()
            cur[h] = got[6, h]

        @pl.when(upper[6])
        def _():
            cur[h] = jnp.zeros((WIDTH, WIDTH), F32)

        split(5, h)
        down_copy(5, h).start()

    def middle(b, h):
        down_copy(b, h).wait_recv()
        cur[h] = cur[h] + got[b, h]
        split(b - 1, h)
        down_copy(b - 1, h).start()

    def three(h):
        down_copy(3, h).wait_recv()
        cur[h] = cur[h] + got[3, h]
        split(2, h)

        @pl.when(is_inner)
        def _():
            join(2, h).start()
            split(1, h)

    def two_join(h):
        @pl.when(is_outer)
        def _():
            join(2, h).wait_recv()
            o[2, h] = o[2, h] + got_join[h]
            down_copy(2, h).start()

    def two(h):
        @pl.when(is_outer)
        def _():
            down_copy(2, h).wait_recv()
            cur[h] = cur[h] + got[2, h]
            split(1, h)
            join(1, h).start()
            split(0, h)
            down_copy(0, h).start()

    def one_join(h):
        @pl.when(is_inner)
        def _():
            join(1, h).wait_recv()
            o[1, h] = o[1, h] + got_join[h]
            down_copy(1, h).start()

    def one(h):
        @pl.when(is_inner)
        def _():
            down_copy(1, h).wait_recv()
            cur[h] = cur[h] + got[1, h]
            split(0, h)
            down_copy(0, h).start()

    def near_backward(h):
        grad = gm[h]
        query = q[:, cols(h)]
        gn = dot(v[:, cols(h)], grad, 1, 1)
        gs = (gn * weight[h]).astype(BF16)
        gkp[h] = dot(gs, query, 1, 0)
        gvp[h] = dot(near[h], grad, 1, 0)
        both = gn * score[h]
        level = table[...]
        for l in range(NEAR_LEVELS):
            part = jnp.sum(jnp.where(level == float(l), both, 0.0), axis=0, keepdims=True)
            gl[l, pl.ds(h, 1), :] = part * level_scale(l)
        mixed[h] = jnp.zeros((WIDTH, TOK), F32)
        query_t = q_t[h].astype(F32)
        for b in range(BITS):
            gl[NEAR_LEVELS + b, pl.ds(h, 1), :] = jnp.zeros((1, TOK), F32)

            @pl.when(upper[b])
            def _(b=b):
                read = dot(recv[b, h].astype(BF16), grad, 1, 1)
                mixed[h] = mixed[h] + read * far_row(b, h)
                part = jnp.sum(query_t * read, axis=0, keepdims=True) * reach[b:b + 1, :]
                gl[NEAR_LEVELS + b, pl.ds(h, 1), :] = part * level_scale(NEAR_LEVELS + b)
        gq[:, cols(h)] = (dot(gs, k[:, cols(h)], 0, 0) + mixed[h].T).astype(BF16)

    def zero(h):
        down_copy(0, h).wait_recv()
        carried = (cur[h] + got[0, h]).astype(BF16)
        held = keep[...]
        kept_v = (v[:, cols(h)].astype(F32) * held).astype(BF16)
        kept_k = (k[:, cols(h)].astype(F32) * held).astype(BF16)
        gk[:, cols(h)] = (gkp[h] + dot(kept_v, carried, 1, 1)).astype(BF16)
        gv[:, cols(h)] = (gvp[h] + dot(kept_k, carried, 1, 0)).astype(BF16)

    events = (
        emit, top, functools.partial(middle, 5), functools.partial(middle, 4), three,
        two_join, two, one_join, one, zero,
    )

    @pl.loop(0, NH + DOWN_LAG[-1])
    def _(step):
        for lag, event in zip(DOWN_LAG, events):
            h = step - lag

            @pl.when((h >= 0) & (h < NH))
            def _(h=h, event=event):
                event(h)

        h = step - 1

        @pl.when((h >= 0) & (h < NH))
        def _():
            near_backward(h)

    swap.wait_send()
    for b in range(BITS):
        only(b, lambda b=b: gate_copy(b).wait_send())
    gate_relay(1).wait_send()

    @pl.loop(0, NH)
    def _(h):
        for b in range(BITS):
            only(b, lambda b=b: up_copy(b, h).wait_send())
        up_relay(1, h).wait_send()
        for b in (0, 3, 4, 5):
            down_copy(b, h).wait_send()
        pl.when(upper[6])(lambda: down_copy(6, h).wait_send())
        pl.when(is_outer)(lambda: down_copy(2, h).wait_send())
        pl.when(is_inner)(lambda: down_copy(1, h).wait_send())
        join(1, h).wait_send()


def per_device(queries, keys, values, segment, level_weight, gain, grad_out):
    vmem = pl.BlockSpec(memory_space=pltpu.VMEM)
    dma = pltpu.SemaphoreType.DMA
    square = (WIDTH, WIDTH)
    wide = jax.ShapeDtypeStruct((TOK, NH * WIDTH), BF16)
    return pl.pallas_call(
        body,
        name="levels",
        out_shape=(wide, wide, wide, wide, jax.ShapeDtypeStruct((LEVELS, NH, TOK), F32)),
        in_specs=[vmem] * 7,
        out_specs=(vmem,) * 5,
        scratch_shapes=[
            pltpu.VMEM(square, F32),
            pltpu.VMEM(square, F32),
            pltpu.VMEM((8, TOK), F32),
            pltpu.VMEM((NH,) + square, F32),
            pltpu.VMEM((BITS, NH) + square, F32),
            pltpu.VMEM((BITS - 1, NH) + square, F32),
            pltpu.VMEM((BITS, 8, 128), F32),
            pltpu.VMEM((BITS, 8, 128), F32),
            pltpu.VMEM((8, 128), F32),
            pltpu.VMEM((NH,) + square, BF16),
            pltpu.VMEM((NH,) + square, BF16),
            pltpu.VMEM((NH,) + square, F32),
            pltpu.VMEM((NH,) + square, F32),
            pltpu.VMEM((NH,) + square, F32),
            pltpu.VMEM((2,) + square, F32),
            pltpu.VMEM((2,) + square, F32),
            pltpu.VMEM((NH,) + square, BF16),
            pltpu.VMEM((BITS, NH) + square, F32),
            pltpu.VMEM((BITS, NH) + square, F32),
            pltpu.VMEM((NH,) + square, F32),
            pltpu.VMEM((NH,) + square, F32),
            pltpu.VMEM((NH,) + square, F32),
            pltpu.VMEM((NH,) + square, F32),
            dma((BITS, NH)), dma((BITS, NH)), dma((NH,)), dma((BITS,)), dma((BITS,)), dma,
            dma((BITS, NH)), dma((BITS, NH)), dma((NH,)), dma((NH,)), dma, dma,
        ],
        compiler_params=pltpu.CompilerParams(
            collective_id=1, has_side_effects=True, vmem_limit_bytes=56 << 20),
    )(queries, keys, values, grad_out, level_weight, segment[None, :], gain[None, :])


def solution(mesh):
    placed = (
        P("tm", "head"), P("tm", "head"), P("tm", "head"), P("tm"),
        P(None, "head", "tm"), P("head"), P("tm", "head"),
    )
    return jax.shard_map(
        per_device,
        mesh=mesh,
        in_specs=placed,
        out_specs=(P("tm", "head"),) * 4 + (P(None, "head", "tm"),),
        check_vma=False,
    )
```

```python
import functools
import jax
import jax.numpy as jnp
from jax import lax
from jax.experimental import pallas as pl
from jax.experimental.pallas import tpu as pltpu
from jax.sharding import PartitionSpec as P

MESH = pl.DeviceIdType.MESH
F32 = jnp.float32
BF16 = jnp.bfloat16
EPSILON = 1e-05
TOK = 128
WIDTH = 128
NH = 16
BITS = 7
NEAR_LEVELS = 8
LEVELS = NEAR_LEVELS + BITS
FEATURES = 4096
UP_LAG = (0, (2, 4), (8, 6), 10, 12, 14, 16)
AHEAD = 3
DOWN_LAG = (0, 2, 4, 6, 8, 10, 12, 14, 16, 16, (19, 18))


def level_scale(l):
    return 2.0 ** (-max(l - 1, 0) / 2)


def dot(a, b, left, right):
    return lax.dot_general(a, b, (((left,), (right,)), ((), ())), preferred_element_type=F32)


def place():
    tm = lax.axis_index("tm")
    z = lax.rem(tm, 8)
    x = lax.rem(lax.div(tm, 8), 4)
    y = lax.div(tm, 32)
    inner = lax.rem(lax.div(z + 1, 2), 2)
    near = tm + 1 - 2 * lax.rem(z, 2)
    across = tm - z + inner * (8 * lax.div(z, 4) + 3 - z) + (1 - inner) * (7 - z)
    x_one = tm + 8 * (1 - 2 * lax.rem(x, 2))
    x_three = tm + 8 * (3 - 2 * x)
    y_one = tm + 32 * (1 - 2 * lax.rem(y, 2))
    y_three = tm + 32 * (3 - 2 * y)
    bits = (
        lax.rem(z, 2), lax.rem(lax.div(z, 2), 2), lax.div(z, 4),
        lax.rem(x, 2), lax.div(x, 2), lax.rem(y, 2), lax.div(y, 2),
    )
    return inner, (near, across, x_one, x_three, y_one, y_three), bits


def remote(src, dst, send, recv, other):
    return pltpu.make_async_remote_copy(
        src_ref=src, dst_ref=dst, send_sem=send, recv_sem=recv,
        device_id=other, device_id_type=MESH,
    )


def body(
    q_in, k_in, v_in, g_in, lw_in, segment, gain,
    normed_out, gq_out, gk_out, gv_out, gl_out,
    q, k, v, g, lw, normed, gq, gk, gv, gl,
    table, keep, far, tails, recv, agg, grecv, gagg, reach, q_t, near, score, weight, mixed, sums, sums_got,
    gm, o, got, got_join, cur, gkp, gvp,
    ssem, rsem, lsem, gss, grs, gls, dssem, drsem, jss, jrs, xss, xrs, in_sem, out_sem, gl_sem,
):
    loads = [
        pltpu.make_async_copy(source, held, in_sem.at[i])
        for i, (source, held) in enumerate(
            ((k_in, k), (v_in, v), (q_in, q), (lw_in, lw), (g_in, g))
        )
    ]
    for load in loads:
        load.start()
    inner, partners, bits = place()
    near_by, across, x_one, x_three, y_one, y_three = partners
    other_core = {"head": 1 - lax.axis_index("head")}
    target = tuple(
        {"tm": p} for p in (near_by, across, across, x_one, x_three, y_one, y_three)
    )
    is_inner = inner == 1
    is_outer = inner == 0
    upper = tuple(bit == 1 for bit in bits)
    lower = tuple(bit == 0 for bit in bits)
    upper_f = tuple(bit.astype(F32) for bit in bits)

    barrier = pltpu.get_barrier_semaphore()
    for p in partners:
        pl.semaphore_signal(barrier, inc=1, device_id={"tm": p}, device_id_type=MESH)
    pl.semaphore_signal(barrier, inc=1, device_id=other_core, device_id_type=MESH)
    pl.semaphore_wait(barrier, 7)

    def cols(h):
        return pl.ds(pl.multiple_of(h * WIDTH, WIDTH), WIDTH)

    def place_out(n, h):
        held, out = ((normed, normed_out), (gq, gq_out), (gk, gk_out), (gv, gv_out))[n]
        return pltpu.make_async_copy(held.at[:, cols(h)], out.at[:, cols(h)], out_sem.at[n, h])

    place_levels = pltpu.make_async_copy(gl, gl_out, gl_sem)

    def only(b, fn):
        if b == 1:
            pl.when(is_inner)(fn)
        elif b == 2:
            pl.when(is_outer)(fn)
        else:
            fn()

    def up_copy(b, h):
        src = tails.at[h] if b == 0 else agg.at[b - 1, h]
        return remote(src, recv.at[b, h], ssem.at[b, h], rsem.at[b, h], target[b])

    def up_relay(b, h):
        return remote(recv.at[b, h], recv.at[b, h], lsem.at[h], rsem.at[b, h], target[0])

    def gate_copy(b):
        return remote(gagg.at[b], grecv.at[b], gss.at[b], grs.at[b], target[b])

    def gate_relay(b):
        return remote(grecv.at[b], grecv.at[b], gls, grs.at[b], target[0])

    def level_row(l, h):
        return lw[l, pl.ds(h, 1), :] * level_scale(l)

    def send_tail(h):
        kept = k[:, cols(h)].astype(F32) * keep[...]
        tails[h] = dot(kept.astype(BF16), v[:, cols(h)], 0, 0)
        up_copy(0, h).start()

    row = segment[...].astype(F32)
    last = row[:, TOK - 1:TOK]
    gagg[0] = jnp.broadcast_to(last, (8, TOK))
    gate_copy(0).start()
    across_t = jnp.broadcast_to(row, (TOK, TOK))
    down_s = across_t.T
    keep[...] = jnp.where(down_s == last, 1.0, 0.0)

    loads[0].wait()
    loads[1].wait()

    @pl.loop(0, AHEAD)
    def _(h):
        send_tail(h)

    at_s = lax.broadcasted_iota(jnp.int32, (TOK, TOK), 0)
    at_t = lax.broadcasted_iota(jnp.int32, (TOK, TOK), 1)
    crossed = jnp.bitwise_xor(at_s, at_t)
    levels = jnp.zeros((TOK, TOK), F32)
    for offset in range(NEAR_LEVELS - 1):
        levels = levels + jnp.where(crossed >= (1 << offset), 1.0, 0.0)
    table[...] = jnp.where((down_s == across_t) & (at_s <= at_t), levels, -1.0)

    def near_forward(h):
        query = q[:, cols(h)]
        s = dot(k[:, cols(h)], query, 1, 1)
        level = table[...]
        w = jnp.zeros((TOK, TOK), F32)
        for l in range(NEAR_LEVELS):
            w = jnp.where(level == float(l), level_row(l, h), w)
        terms = (s * w).astype(BF16)
        score[h] = s
        weight[h] = w
        near[h] = terms
        q_t[h] = query.T
        mixed[h] = dot(terms, v[:, cols(h)], 0, 0)

    def up_event(b, h):
        @pl.when(h == 0)
        def _():
            gate_copy(b).wait_recv()
            if b in (1, 2):
                only(b, lambda: gate_relay(b).start())
            if b < BITS - 1:
                gagg[b + 1] = gagg[b] * upper_f[b] + grecv[b] * (1.0 - upper_f[b])
                only(b + 1, lambda: gate_copy(b + 1).start())
            hit = jnp.where(segment[...].astype(F32) == grecv[b, 0:1, :], 1.0, 0.0)
            reach[b:b + 1, :] = hit * upper_f[b]

        up_copy(b, h).wait_recv()
        if b in (1, 2):
            only(b, lambda: up_relay(b, h).start())
        if b < BITS - 1:
            same = jnp.where(grecv[b, 0:1, :] == gagg[b, 0:1, :], 1.0, 0.0)
            mine_by = upper_f[b] + (1.0 - upper_f[b]) * same
            got_by = (1.0 - upper_f[b]) + upper_f[b] * same
            mine = tails[h] if b == 0 else agg[b - 1, h]
            agg[b, h] = mine * mine_by + recv[b, h] * got_by
            only(b + 1, lambda: up_copy(b + 1, h).start())

    def far_read(h):
        for b in range(BITS):
            far[b:b + 1, :] = level_row(NEAR_LEVELS + b, h)
        by_t = (far[...] * reach[...]).T
        query = q[:, cols(h)].astype(F32)
        for b in range(BITS):
            @pl.when(upper[b])
            def _(b=b):
                scaled_q = (query * by_t[:, b:b + 1]).astype(BF16)
                mixed[h] = mixed[h] + dot(scaled_q, recv[b, h].astype(BF16), 1, 0)
        m = mixed[h]
        sums[0] = sums[0] + m * m
        sums[1] = sums[1] + m * g[:, cols(h)].astype(F32) * gain[:, cols(h)]

    for load in loads[2:]:
        load.wait()
    sums[...] = jnp.zeros_like(sums)
    reach[...] = jnp.zeros_like(reach)
    far[...] = jnp.zeros_like(far)

    @pl.loop(0, NH + UP_LAG[-1])
    def _(step):
        @pl.when(step + AHEAD < NH)
        def _():
            send_tail(step + AHEAD)

        for b in range(BITS):
            lag = UP_LAG[b]
            if isinstance(lag, tuple):
                lag = lag[0] * inner + lag[1] * (1 - inner)
            h = step - lag

            @pl.when((h >= 0) & (h < NH))
            def _(b=b, h=h):
                up_event(b, h)

        @pl.when(step < NH)
        def _():
            near_forward(step)

        h = step - UP_LAG[-1]

        @pl.when(h >= 0)
        def _():
            far_read(h)

    swap = remote(sums, sums_got, xss, xrs, other_core)
    swap.start()
    swap.wait_recv()
    squares = jnp.sum(sums[0] + sums_got[0], axis=1, keepdims=True)
    project = jnp.sum(sums[1] + sums_got[1], axis=1, keepdims=True)
    radius = jnp.sqrt(squares / FEATURES + EPSILON)
    inverse = 1.0 / radius
    pull = project * inverse * inverse * inverse / FEATURES

    def down_copy(b, h):
        return remote(o.at[b, h], got.at[b, h], dssem.at[b, h], drsem.at[b, h], target[b])

    def join(b, h):
        return remote(o.at[b, h], got_join.at[h], jss.at[h], jrs.at[h], target[0])

    def far_row(b, h):
        return level_row(NEAR_LEVELS + b, h) * reach[b:b + 1, :]

    def far_grad(b, h):
        scaled_q = (q_t[h].astype(F32) * far_row(b, h)).astype(BF16)
        return dot(scaled_q, gm[h], 1, 0)

    def split(b, h):
        same = jnp.where(grecv[b, 0:1, :] == gagg[b, 0:1, :], 1.0, 0.0)

        @pl.when(upper[b])
        def _():
            o[b, h] = cur[h] * same + far_grad(b, h)

        @pl.when(lower[b])
        def _():
            o[b, h] = cur[h]
            cur[h] = cur[h] * same

    def emit(h):
        m = mixed[h]
        scale = gain[:, cols(h)]
        normed[:, cols(h)] = (m * inverse * scale).astype(BF16)
        place_out(0, h).start()
        gm[h] = (scale * g[:, cols(h)].astype(F32) * inverse - m * pull).astype(BF16)

        @pl.when(upper[6])
        def _():
            o[6, h] = far_grad(6, h)
            down_copy(6, h).start()

    def top(h):
        @pl.when(lower[6])
        def _():
            down_copy(6, h).wait_recv()
            cur[h] = got[6, h]

        @pl.when(upper[6])
        def _():
            cur[h] = jnp.zeros((WIDTH, WIDTH), F32)

        split(5, h)
        down_copy(5, h).start()

    def middle(b, h):
        down_copy(b, h).wait_recv()
        cur[h] = cur[h] + got[b, h]
        split(b - 1, h)
        down_copy(b - 1, h).start()

    def three(h):
        down_copy(3, h).wait_recv()
        cur[h] = cur[h] + got[3, h]
        split(2, h)

        @pl.when(is_inner)
        def _():
            join(2, h).start()
            split(1, h)

    def two_join(h):
        @pl.when(is_outer)
        def _():
            join(2, h).wait_recv()
            o[2, h] = o[2, h] + got_join[h]
            down_copy(2, h).start()

    def two(h):
        @pl.when(is_outer)
        def _():
            down_copy(2, h).wait_recv()
            cur[h] = cur[h] + got[2, h]
            split(1, h)
            join(1, h).start()
            split(0, h)

    def late(h):
        @pl.when(is_outer)
        def _():
            down_copy(0, h).start()

    def one_join(h):
        @pl.when(is_inner)
        def _():
            join(1, h).wait_recv()
            o[1, h] = o[1, h] + got_join[h]
            down_copy(1, h).start()

    def one(h):
        @pl.when(is_inner)
        def _():
            down_copy(1, h).wait_recv()
            cur[h] = cur[h] + got[1, h]
            split(0, h)
            down_copy(0, h).start()

    def near_backward(h):
        grad = gm[h]
        query = q[:, cols(h)]
        gn = dot(v[:, cols(h)], grad, 1, 1)
        gs = (gn * weight[h]).astype(BF16)
        gkp[h] = dot(gs, query, 1, 0)
        gvp[h] = dot(near[h], grad, 1, 0)
        both = gn * score[h]
        level = table[...]
        for l in range(NEAR_LEVELS):
            part = jnp.sum(jnp.where(level == float(l), both, 0.0), axis=0, keepdims=True)
            gl[l, pl.ds(h, 1), :] = part * level_scale(l)
        mixed[h] = jnp.zeros((WIDTH, TOK), F32)
        query_t = q_t[h].astype(F32)
        for b in range(BITS):
            gl[NEAR_LEVELS + b, pl.ds(h, 1), :] = jnp.zeros((1, TOK), F32)

            @pl.when(upper[b])
            def _(b=b):
                read = dot(recv[b, h].astype(BF16), grad, 1, 1)
                mixed[h] = mixed[h] + read * far_row(b, h)
                part = jnp.sum(query_t * read, axis=0, keepdims=True) * reach[b:b + 1, :]
                gl[NEAR_LEVELS + b, pl.ds(h, 1), :] = part * level_scale(NEAR_LEVELS + b)
        gq[:, cols(h)] = (dot(gs, k[:, cols(h)], 0, 0) + mixed[h].T).astype(BF16)
        place_out(1, h).start()

        @pl.when(h == NH - 1)
        def _():
            place_levels.start()

    def zero(h):
        down_copy(0, h).wait_recv()
        carried = (cur[h] + got[0, h]).astype(BF16)
        held = keep[...]
        kept_v = (v[:, cols(h)].astype(F32) * held).astype(BF16)
        kept_k = (k[:, cols(h)].astype(F32) * held).astype(BF16)
        gk[:, cols(h)] = (gkp[h] + dot(kept_v, carried, 1, 1)).astype(BF16)
        gv[:, cols(h)] = (gvp[h] + dot(kept_k, carried, 1, 0)).astype(BF16)
        place_out(2, h).start()
        place_out(3, h).start()

    events = (
        emit, top, functools.partial(middle, 5), functools.partial(middle, 4), three,
        two_join, two, one_join, one, late, zero,
    )

    @pl.loop(0, NH + max(DOWN_LAG[-1]))
    def _(step):
        for lag, event in zip(DOWN_LAG, events):
            if isinstance(lag, tuple):
                lag = lag[0] * inner + lag[1] * (1 - inner)
            h = step - lag

            @pl.when((h >= 0) & (h < NH))
            def _(h=h, event=event):
                event(h)

        h = step - 1

        @pl.when((h >= 0) & (h < NH))
        def _():
            near_backward(h)

    place_levels.wait()
    swap.wait_send()
    for b in range(BITS):
        only(b, lambda b=b: gate_copy(b).wait_send())
    gate_relay(1).wait_send()

    @pl.loop(0, NH)
    def _(h):
        for b in range(BITS):
            only(b, lambda b=b: up_copy(b, h).wait_send())
        up_relay(1, h).wait_send()
        for b in (0, 3, 4, 5):
            down_copy(b, h).wait_send()
        pl.when(upper[6])(lambda: down_copy(6, h).wait_send())
        pl.when(is_outer)(lambda: down_copy(2, h).wait_send())
        pl.when(is_inner)(lambda: down_copy(1, h).wait_send())
        join(1, h).wait_send()
        for n in range(4):
            place_out(n, h).wait()


def hand_over(*refs):
    for source, out in zip(refs[:5], refs[5:]):
        out[...] = source[...]


def per_device(queries, keys, values, segment, level_weight, gain, grad_out):
    vmem = pl.BlockSpec(memory_space=pltpu.VMEM)
    dma = pltpu.SemaphoreType.DMA
    square = (WIDTH, WIDTH)
    wide = jax.ShapeDtypeStruct((TOK, NH * WIDTH), BF16)
    away = pl.BlockSpec(memory_space=pl.ANY)
    shapes = (wide, wide, wide, wide, jax.ShapeDtypeStruct((LEVELS, NH, TOK), F32))
    made = pl.pallas_call(
        body,
        name="levels",
        out_shape=shapes,
        in_specs=[away] * 5 + [vmem] * 2,
        out_specs=(away,) * 5,
        scratch_shapes=[
            pltpu.VMEM((TOK, NH * WIDTH), BF16),
            pltpu.VMEM((TOK, NH * WIDTH), BF16),
            pltpu.VMEM((TOK, NH * WIDTH), BF16),
            pltpu.VMEM((TOK, NH * WIDTH), BF16),
            pltpu.VMEM((LEVELS, NH, TOK), F32),
            pltpu.VMEM((TOK, NH * WIDTH), BF16),
            pltpu.VMEM((TOK, NH * WIDTH), BF16),
            pltpu.VMEM((TOK, NH * WIDTH), BF16),
            pltpu.VMEM((TOK, NH * WIDTH), BF16),
            pltpu.VMEM((LEVELS, NH, TOK), F32),
            pltpu.VMEM(square, F32),
            pltpu.VMEM(square, F32),
            pltpu.VMEM((8, TOK), F32),
            pltpu.VMEM((NH,) + square, F32),
            pltpu.VMEM((BITS, NH) + square, F32),
            pltpu.VMEM((BITS - 1, NH) + square, F32),
            pltpu.VMEM((BITS, 8, 128), F32),
            pltpu.VMEM((BITS, 8, 128), F32),
            pltpu.VMEM((8, 128), F32),
            pltpu.VMEM((NH,) + square, BF16),
            pltpu.VMEM((NH,) + square, BF16),
            pltpu.VMEM((NH,) + square, F32),
            pltpu.VMEM((NH,) + square, F32),
            pltpu.VMEM((NH,) + square, F32),
            pltpu.VMEM((2,) + square, F32),
            pltpu.VMEM((2,) + square, F32),
            pltpu.VMEM((NH,) + square, BF16),
            pltpu.VMEM((BITS, NH) + square, F32),
            pltpu.VMEM((BITS, NH) + square, F32),
            pltpu.VMEM((NH,) + square, F32),
            pltpu.VMEM((NH,) + square, F32),
            pltpu.VMEM((NH,) + square, F32),
            pltpu.VMEM((NH,) + square, F32),
            dma((BITS, NH)), dma((BITS, NH)), dma((NH,)), dma((BITS,)), dma((BITS,)), dma,
            dma((BITS, NH)), dma((BITS, NH)), dma((NH,)), dma((NH,)), dma, dma,
            dma((5,)), dma((4, NH)), dma,
        ],
        compiler_params=pltpu.CompilerParams(
            collective_id=1, has_side_effects=True, vmem_limit_bytes=56 << 20),
    )(queries, keys, values, grad_out, level_weight, segment[None, :], gain[None, :])
    strip = pl.BlockSpec((TOK // 4, NH * WIDTH), lambda i: (i, 0))
    whole = pl.BlockSpec((LEVELS, NH, TOK), lambda i: (0, 0, 0))
    return pl.pallas_call(
        hand_over,
        name="hand_over",
        grid=(4,),
        out_shape=shapes,
        in_specs=[strip] * 4 + [whole],
        out_specs=[strip] * 4 + [whole],
    )(*made)


def solution(mesh):
    placed = (
        P("tm", "head"), P("tm", "head"), P("tm", "head"), P("tm"),
        P(None, "head", "tm"), P("head"), P("tm", "head"),
    )
    return jax.shard_map(
        per_device,
        mesh=mesh,
        in_specs=placed,
        out_specs=(P("tm", "head"),) * 4 + (P(None, "head", "tm"),),
        check_vma=False,
    )
```

```python
import functools
import jax
import jax.numpy as jnp
from jax import lax
from jax.experimental import pallas as pl
from jax.experimental.pallas import tpu as pltpu
from jax.sharding import PartitionSpec as P

MESH = pl.DeviceIdType.MESH
F32 = jnp.float32
BF16 = jnp.bfloat16
EPSILON = 1e-05
TOK = 128
WIDTH = 128
NH = 16
BITS = 7
NEAR_LEVELS = 8
LEVELS = NEAR_LEVELS + BITS
FEATURES = 4096
UP_LAG = (0, (2, 4), (8, 6), 10, 12, 14, 16)
AHEAD = 3
DOWN_LAG = (0, 2, 4, 6, 8, 10, 12, 14, 16, 16, (19, 18))


def level_scale(l):
    return 2.0 ** (-max(l - 1, 0) / 2)


def dot(a, b, left, right):
    return lax.dot_general(a, b, (((left,), (right,)), ((), ())), preferred_element_type=F32)


def place():
    tm = lax.axis_index("tm")
    z = lax.rem(tm, 8)
    x = lax.rem(lax.div(tm, 8), 4)
    y = lax.div(tm, 32)
    inner = lax.rem(lax.div(z + 1, 2), 2)
    near = tm + 1 - 2 * lax.rem(z, 2)
    across = tm - z + inner * (8 * lax.div(z, 4) + 3 - z) + (1 - inner) * (7 - z)
    x_one = tm + 8 * (1 - 2 * lax.rem(x, 2))
    x_three = tm + 8 * (3 - 2 * x)
    y_one = tm + 32 * (1 - 2 * lax.rem(y, 2))
    y_three = tm + 32 * (3 - 2 * y)
    bits = (
        lax.rem(z, 2), lax.rem(lax.div(z, 2), 2), lax.div(z, 4),
        lax.rem(x, 2), lax.div(x, 2), lax.rem(y, 2), lax.div(y, 2),
    )
    return inner, (near, across, x_one, x_three, y_one, y_three), bits


def remote(src, dst, send, recv, other):
    return pltpu.make_async_remote_copy(
        src_ref=src, dst_ref=dst, send_sem=send, recv_sem=recv,
        device_id=other, device_id_type=MESH,
    )


def body(
    q_in, k_in, v_in, g_in, lw_in, segment, gain,
    normed_out, gq_out, gk_out, gv_out, gl_out,
    q, k, v, g, lw, normed, gq, gk, gv, gl,
    table, keep, far, tails, recv, agg, grecv, gagg, reach, q_t, near, score, weight, mixed, sums, sums_got,
    gm, o, got, got_join, cur, gkp, gvp,
    ssem, rsem, lsem, gss, grs, gls, dssem, drsem, jss, jrs, xss, xrs, in_sem, out_sem, gl_sem,
):
    loads = [
        pltpu.make_async_copy(source, held, in_sem.at[i])
        for i, (source, held) in enumerate(
            ((k_in, k), (v_in, v), (q_in, q), (lw_in, lw), (g_in, g))
        )
    ]
    for load in loads:
        load.start()
    inner, partners, bits = place()
    near_by, across, x_one, x_three, y_one, y_three = partners
    other_core = {"head": 1 - lax.axis_index("head")}
    target = tuple(
        {"tm": p} for p in (near_by, across, across, x_one, x_three, y_one, y_three)
    )
    is_inner = inner == 1
    is_outer = inner == 0
    upper = tuple(bit == 1 for bit in bits)
    lower = tuple(bit == 0 for bit in bits)
    upper_f = tuple(bit.astype(F32) for bit in bits)

    barrier = pltpu.get_barrier_semaphore()
    for p in partners:
        pl.semaphore_signal(barrier, inc=1, device_id={"tm": p}, device_id_type=MESH)
    pl.semaphore_signal(barrier, inc=1, device_id=other_core, device_id_type=MESH)
    pl.semaphore_wait(barrier, 7)

    def cols(h):
        return pl.ds(pl.multiple_of(h * WIDTH, WIDTH), WIDTH)

    def place_out(n, h):
        held, out = ((normed, normed_out), (gq, gq_out), (gk, gk_out), (gv, gv_out))[n]
        return pltpu.make_async_copy(held.at[:, cols(h)], out.at[:, cols(h)], out_sem.at[n, h])

    place_levels = pltpu.make_async_copy(gl, gl_out, gl_sem)

    def only(b, fn):
        if b == 1:
            pl.when(is_inner)(fn)
        elif b == 2:
            pl.when(is_outer)(fn)
        else:
            fn()

    def up_copy(b, h):
        src = tails.at[h] if b == 0 else agg.at[b - 1, h]
        return remote(src, recv.at[b, h], ssem.at[b, h], rsem.at[b, h], target[b])

    def up_relay(b, h):
        return remote(recv.at[b, h], recv.at[b, h], lsem.at[h], rsem.at[b, h], target[0])

    def gate_copy(b):
        return remote(gagg.at[b], grecv.at[b], gss.at[b], grs.at[b], target[b])

    def gate_relay(b):
        return remote(grecv.at[b], grecv.at[b], gls, grs.at[b], target[0])

    def level_row(l, h):
        return lw[l, pl.ds(h, 1), :] * level_scale(l)

    def send_tail(h):
        kept = k[:, cols(h)].astype(F32) * keep[...]
        tails[h] = dot(kept.astype(BF16), v[:, cols(h)], 0, 0)
        up_copy(0, h).start()

    row = segment[...].astype(F32)
    last = row[:, TOK - 1:TOK]
    gagg[0] = jnp.broadcast_to(last, (8, TOK))
    gate_copy(0).start()
    across_t = jnp.broadcast_to(row, (TOK, TOK))
    down_s = across_t.T
    keep[...] = jnp.where(down_s == last, 1.0, 0.0)

    loads[0].wait()
    loads[1].wait()

    @pl.loop(0, AHEAD)
    def _(h):
        send_tail(h)

    at_s = lax.broadcasted_iota(jnp.int32, (TOK, TOK), 0)
    at_t = lax.broadcasted_iota(jnp.int32, (TOK, TOK), 1)
    crossed = jnp.bitwise_xor(at_s, at_t)
    levels = jnp.zeros((TOK, TOK), F32)
    for offset in range(NEAR_LEVELS - 1):
        levels = levels + jnp.where(crossed >= (1 << offset), 1.0, 0.0)
    table[...] = jnp.where((down_s == across_t) & (at_s <= at_t), levels, -1.0)

    def near_forward(h):
        query = q[:, cols(h)]
        s = dot(k[:, cols(h)], query, 1, 1)
        level = table[...]
        w = jnp.zeros((TOK, TOK), F32)
        for l in range(NEAR_LEVELS):
            w = jnp.where(level == float(l), level_row(l, h), w)
        terms = (s * w).astype(BF16)
        score[h] = s
        weight[h] = w
        near[h] = terms
        q_t[h] = query.T
        mixed[h] = dot(terms, v[:, cols(h)], 0, 0)

    def up_event(b, h):
        @pl.when(h == 0)
        def _():
            gate_copy(b).wait_recv()
            if b in (1, 2):
                only(b, lambda: gate_relay(b).start())
            if b < BITS - 1:
                gagg[b + 1] = gagg[b] * upper_f[b] + grecv[b] * (1.0 - upper_f[b])
                only(b + 1, lambda: gate_copy(b + 1).start())
            hit = jnp.where(segment[...].astype(F32) == grecv[b, 0:1, :], 1.0, 0.0)
            reach[b:b + 1, :] = hit * upper_f[b]

        up_copy(b, h).wait_recv()
        if b in (1, 2):
            only(b, lambda: up_relay(b, h).start())
        if b < BITS - 1:
            same = jnp.where(grecv[b, 0:1, :] == gagg[b, 0:1, :], 1.0, 0.0)
            mine_by = upper_f[b] + (1.0 - upper_f[b]) * same
            got_by = (1.0 - upper_f[b]) + upper_f[b] * same
            mine = tails[h] if b == 0 else agg[b - 1, h]
            agg[b, h] = mine * mine_by + recv[b, h] * got_by
            only(b + 1, lambda: up_copy(b + 1, h).start())

    def far_read(h):
        for b in range(BITS):
            far[b:b + 1, :] = level_row(NEAR_LEVELS + b, h)
        by_t = (far[...] * reach[...]).T
        query = q[:, cols(h)].astype(F32)
        m = mixed[h]
        for b in range(BITS):
            scaled_q = (query * by_t[:, b:b + 1]).astype(BF16)
            m = m + dot(scaled_q, recv[b, h].astype(BF16), 1, 0)
        mixed[h] = m
        sums[0] = sums[0] + m * m
        sums[1] = sums[1] + m * g[:, cols(h)].astype(F32) * gain[:, cols(h)]

    for load in loads[2:]:
        load.wait()
    sums[...] = jnp.zeros_like(sums)
    reach[...] = jnp.zeros_like(reach)
    far[...] = jnp.zeros_like(far)

    @pl.loop(0, NH + UP_LAG[-1])
    def _(step):
        @pl.when(step + AHEAD < NH)
        def _():
            send_tail(step + AHEAD)

        for b in range(BITS):
            lag = UP_LAG[b]
            if isinstance(lag, tuple):
                lag = lag[0] * inner + lag[1] * (1 - inner)
            h = step - lag

            @pl.when((h >= 0) & (h < NH))
            def _(b=b, h=h):
                up_event(b, h)

        @pl.when(step < NH)
        def _():
            near_forward(step)

        h = step - UP_LAG[-1]

        @pl.when(h >= 0)
        def _():
            far_read(h)

    swap = remote(sums, sums_got, xss, xrs, other_core)
    swap.start()
    swap.wait_recv()
    squares = jnp.sum(sums[0] + sums_got[0], axis=1, keepdims=True)
    project = jnp.sum(sums[1] + sums_got[1], axis=1, keepdims=True)
    radius = jnp.sqrt(squares / FEATURES + EPSILON)
    inverse = 1.0 / radius
    pull = project * inverse * inverse * inverse / FEATURES

    def down_copy(b, h):
        return remote(o.at[b, h], got.at[b, h], dssem.at[b, h], drsem.at[b, h], target[b])

    def join(b, h):
        return remote(o.at[b, h], got_join.at[h], jss.at[h], jrs.at[h], target[0])

    def far_row(b, h):
        return level_row(NEAR_LEVELS + b, h) * reach[b:b + 1, :]

    def far_grad(b, h):
        scaled_q = (q_t[h].astype(F32) * far_row(b, h)).astype(BF16)
        return dot(scaled_q, gm[h], 1, 0)

    def split(b, h):
        same = jnp.where(grecv[b, 0:1, :] == gagg[b, 0:1, :], 1.0, 0.0)
        leave_by = upper_f[b] * same + (1.0 - upper_f[b])
        stay_by = upper_f[b] + (1.0 - upper_f[b]) * same
        carried = cur[h]
        o[b, h] = o[b, h] + carried * leave_by
        cur[h] = carried * stay_by

    def emit(h):
        m = mixed[h]
        scale = gain[:, cols(h)]
        normed[:, cols(h)] = (m * inverse * scale).astype(BF16)
        place_out(0, h).start()
        gm[h] = (scale * g[:, cols(h)].astype(F32) * inverse - m * pull).astype(BF16)

        for b in reversed(range(BITS)):
            o[b, h] = far_grad(b, h)
            if b == BITS - 1:
                pl.when(upper[6])(lambda: down_copy(6, h).start())

    def top(h):
        @pl.when(lower[6])
        def _():
            down_copy(6, h).wait_recv()
            cur[h] = got[6, h]

        @pl.when(upper[6])
        def _():
            cur[h] = jnp.zeros((WIDTH, WIDTH), F32)

        split(5, h)
        down_copy(5, h).start()

    def middle(b, h):
        down_copy(b, h).wait_recv()
        cur[h] = cur[h] + got[b, h]
        split(b - 1, h)
        down_copy(b - 1, h).start()

    def three(h):
        down_copy(3, h).wait_recv()
        cur[h] = cur[h] + got[3, h]
        split(2, h)

        @pl.when(is_inner)
        def _():
            join(2, h).start()
            split(1, h)

    def two_join(h):
        @pl.when(is_outer)
        def _():
            join(2, h).wait_recv()
            o[2, h] = o[2, h] + got_join[h]
            down_copy(2, h).start()

    def two(h):
        @pl.when(is_outer)
        def _():
            down_copy(2, h).wait_recv()
            cur[h] = cur[h] + got[2, h]
            split(1, h)
            join(1, h).start()
            split(0, h)

    def late(h):
        @pl.when(is_outer)
        def _():
            down_copy(0, h).start()

    def one_join(h):
        @pl.when(is_inner)
        def _():
            join(1, h).wait_recv()
            o[1, h] = o[1, h] + got_join[h]
            down_copy(1, h).start()

    def one(h):
        @pl.when(is_inner)
        def _():
            down_copy(1, h).wait_recv()
            cur[h] = cur[h] + got[1, h]
            split(0, h)
            down_copy(0, h).start()

    def near_backward(h):
        grad = gm[h]
        query = q[:, cols(h)]
        gn = dot(v[:, cols(h)], grad, 1, 1)
        gs = (gn * weight[h]).astype(BF16)
        gkp[h] = dot(gs, query, 1, 0)
        gvp[h] = dot(near[h], grad, 1, 0)
        both = gn * score[h]
        level = table[...]
        for l in range(NEAR_LEVELS):
            part = jnp.sum(jnp.where(level == float(l), both, 0.0), axis=0, keepdims=True)
            gl[l, pl.ds(h, 1), :] = part * level_scale(l)
        far_t = jnp.zeros((WIDTH, TOK), F32)
        query_t = q_t[h].astype(F32)
        for b in range(BITS):
            read = dot(recv[b, h].astype(BF16), grad, 1, 1)
            far_t = far_t + read * far_row(b, h)
            part = jnp.sum(query_t * read, axis=0, keepdims=True) * reach[b:b + 1, :]
            gl[NEAR_LEVELS + b, pl.ds(h, 1), :] = part * level_scale(NEAR_LEVELS + b)
        gq[:, cols(h)] = (dot(gs, k[:, cols(h)], 0, 0) + far_t.T).astype(BF16)
        place_out(1, h).start()

        @pl.when(h == NH - 1)
        def _():
            place_levels.start()

    def zero(h):
        down_copy(0, h).wait_recv()
        carried = (cur[h] + got[0, h]).astype(BF16)
        held = keep[...]
        kept_v = (v[:, cols(h)].astype(F32) * held).astype(BF16)
        kept_k = (k[:, cols(h)].astype(F32) * held).astype(BF16)
        gk[:, cols(h)] = (gkp[h] + dot(kept_v, carried, 1, 1)).astype(BF16)
        gv[:, cols(h)] = (gvp[h] + dot(kept_k, carried, 1, 0)).astype(BF16)
        place_out(2, h).start()
        place_out(3, h).start()

    events = (
        emit, top, functools.partial(middle, 5), functools.partial(middle, 4), three,
        two_join, two, one_join, one, late, zero,
    )

    @pl.loop(0, NH + max(DOWN_LAG[-1]))
    def _(step):
        for lag, event in zip(DOWN_LAG, events):
            if isinstance(lag, tuple):
                lag = lag[0] * inner + lag[1] * (1 - inner)
            h = step - lag

            @pl.when((h >= 0) & (h < NH))
            def _(h=h, event=event):
                event(h)

        h = step - 1

        @pl.when((h >= 0) & (h < NH))
        def _():
            near_backward(h)

    place_levels.wait()
    swap.wait_send()
    for b in range(BITS):
        only(b, lambda b=b: gate_copy(b).wait_send())
    gate_relay(1).wait_send()

    @pl.loop(0, NH)
    def _(h):
        for b in range(BITS):
            only(b, lambda b=b: up_copy(b, h).wait_send())
        up_relay(1, h).wait_send()
        for b in (0, 3, 4, 5):
            down_copy(b, h).wait_send()
        pl.when(upper[6])(lambda: down_copy(6, h).wait_send())
        pl.when(is_outer)(lambda: down_copy(2, h).wait_send())
        pl.when(is_inner)(lambda: down_copy(1, h).wait_send())
        join(1, h).wait_send()
        for n in range(4):
            place_out(n, h).wait()


def hand_over(*refs):
    held, read_sem, write_sem = refs[10:15], refs[15], refs[16]
    reads = [pltpu.make_async_copy(refs[i], held[i], read_sem.at[i]) for i in range(5)]
    writes = [pltpu.make_async_copy(held[i], refs[5 + i], write_sem.at[i]) for i in range(5)]
    for read in reads:
        read.start()
    for read, write in zip(reads, writes):
        read.wait()
        write.start()
    for write in writes:
        write.wait()


def per_device(queries, keys, values, segment, level_weight, gain, grad_out):
    vmem = pl.BlockSpec(memory_space=pltpu.VMEM)
    dma = pltpu.SemaphoreType.DMA
    square = (WIDTH, WIDTH)
    wide = jax.ShapeDtypeStruct((TOK, NH * WIDTH), BF16)
    away = pl.BlockSpec(memory_space=pl.ANY)
    shapes = (wide, wide, wide, wide, jax.ShapeDtypeStruct((LEVELS, NH, TOK), F32))
    made = pl.pallas_call(
        body,
        name="levels",
        out_shape=shapes,
        in_specs=[away] * 5 + [vmem] * 2,
        out_specs=(away,) * 5,
        scratch_shapes=[
            pltpu.VMEM((TOK, NH * WIDTH), BF16),
            pltpu.VMEM((TOK, NH * WIDTH), BF16),
            pltpu.VMEM((TOK, NH * WIDTH), BF16),
            pltpu.VMEM((TOK, NH * WIDTH), BF16),
            pltpu.VMEM((LEVELS, NH, TOK), F32),
            pltpu.VMEM((TOK, NH * WIDTH), BF16),
            pltpu.VMEM((TOK, NH * WIDTH), BF16),
            pltpu.VMEM((TOK, NH * WIDTH), BF16),
            pltpu.VMEM((TOK, NH * WIDTH), BF16),
            pltpu.VMEM((LEVELS, NH, TOK), F32),
            pltpu.VMEM(square, F32),
            pltpu.VMEM(square, F32),
            pltpu.VMEM((8, TOK), F32),
            pltpu.VMEM((NH,) + square, F32),
            pltpu.VMEM((BITS, NH) + square, F32),
            pltpu.VMEM((BITS - 1, NH) + square, F32),
            pltpu.VMEM((BITS, 8, 128), F32),
            pltpu.VMEM((BITS, 8, 128), F32),
            pltpu.VMEM((8, 128), F32),
            pltpu.VMEM((NH,) + square, BF16),
            pltpu.VMEM((NH,) + square, BF16),
            pltpu.VMEM((NH,) + square, F32),
            pltpu.VMEM((NH,) + square, F32),
            pltpu.VMEM((NH,) + square, F32),
            pltpu.VMEM((2,) + square, F32),
            pltpu.VMEM((2,) + square, F32),
            pltpu.VMEM((NH,) + square, BF16),
            pltpu.VMEM((BITS, NH) + square, F32),
            pltpu.VMEM((BITS, NH) + square, F32),
            pltpu.VMEM((NH,) + square, F32),
            pltpu.VMEM((NH,) + square, F32),
            pltpu.VMEM((NH,) + square, F32),
            pltpu.VMEM((NH,) + square, F32),
            dma((BITS, NH)), dma((BITS, NH)), dma((NH,)), dma((BITS,)), dma((BITS,)), dma,
            dma((BITS, NH)), dma((BITS, NH)), dma((NH,)), dma((NH,)), dma, dma,
            dma((5,)), dma((4, NH)), dma,
        ],
        compiler_params=pltpu.CompilerParams(
            collective_id=1, has_side_effects=True, vmem_limit_bytes=56 << 20),
    )(queries, keys, values, grad_out, level_weight, segment[None, :], gain[None, :])
    return pl.pallas_call(
        hand_over,
        name="hand_over",
        out_shape=shapes,
        in_specs=[away] * 5,
        out_specs=(away,) * 5,
        scratch_shapes=[pltpu.VMEM(shape.shape, shape.dtype) for shape in shapes] + [dma((5,)), dma((5,))],
    )(*made)


def solution(mesh):
    placed = (
        P("tm", "head"), P("tm", "head"), P("tm", "head"), P("tm"),
        P(None, "head", "tm"), P("head"), P("tm", "head"),
    )
    return jax.shard_map(
        per_device,
        mesh=mesh,
        in_specs=placed,
        out_specs=(P("tm", "head"),) * 4 + (P(None, "head", "tm"),),
        check_vma=False,
    )
```
